32 devices in a mesh: leaf: 8 (over z, x), rows: 4 (over y, core).
Axes of the slice: x: 2, y: 2, z: 4, core: 2. Of those that a mesh axis runs over, the one named last changes fastest.
Arguments:
- right_side: float32 [8, 32768], P(None, ('leaf', 'rows')), may hold values from -6 to 6
- diagonal: float32 [32768], P(('leaf', 'rows')), may hold values from 0.5 to 4
- tree_order: int32 [32768], P(('leaf', 'rows')), may hold values from 0 to 32767, as said below
- mid_perm: int32 [8], replicated, may hold values from 0 to 7, each once
- col_factor: bfloat16 [32768, 384], P(('leaf', 'rows')), may hold values from -0.1875 to 0.1875
- mid_factor: bfloat16 [3072, 768], P('leaf', 'rows'), may hold values from -0.15625 to 0.15625
- pre_factor: bfloat16 [3072, 768], P('leaf', 'rows'), may hold values from -0.15625 to 0.15625
- row_factor: bfloat16 [48, 32768], P(None, ('leaf', 'rows')), may hold values from -0.875 to 0.875
Outputs:
- solution: float32 [8, 32768], P(None, ('leaf', 'rows'))
- residual: float32 [8, 32768], P(None, ('leaf', 'rows'))
The draws below stay inside these ranges and needn't reach their ends.
Inputs may be any that keep to these rules, and one draw needn't show every extreme that they name: `tree_order`: each aligned run of 1024 entries, the run starting at b * 1024, is a permutation of b * 1024 to (b + 1) * 1024 - 1. `mid_perm`: a permutation of 0 to 7.
All inputs are finite; a program needn't handle non-finite values.
Results may differ from the reference program's by a relative error of at most 0.025.
Values may be sent and summed in bfloat16 or wider, within the bound.
A program may use at most 64 MiB of HBM per device.

```python
import math
import jax
import jax.numpy as jnp
from jax import lax

PTS = 1024
RANK = 48
RHS = 8
ITERS = 2
LEAVES = 8
ROWB = 4
NPTS = 32768
N_LEAF = 8
N_ROWS = 4


def draw_tree_order(key, part):
    blocks = NPTS // PTS
    upper_bound = (1 << 30) // PTS
    scores = jax.random.randint(jax.random.fold_in(key, 11), (blocks, PTS), 0, upper_bound, dtype=jnp.int32)
    scores = scores * PTS + jnp.arange(PTS, dtype=jnp.int32)[None, :]
    within = jnp.argsort(scores, axis=1).astype(jnp.int32)
    starts = (jnp.arange(blocks, dtype=jnp.int32) * PTS)[:, None]
    return (within + starts).reshape(NPTS).astype(jnp.int32)


def steps_of(own_key, dims, pieces, smallest, largest):
    gain, own = 1.0, jax.random.fold_in(own_key, 6)
    for dim, parts in pieces:
        draws = jnp.exp(jax.random.uniform(jax.random.fold_in(own, dim), (parts,), jnp.float32, smallest / len(pieces), largest / len(pieces)))
        gain = gain * jnp.repeat(draws, dims[dim] // parts).reshape([-1 if axis == dim else 1 for axis in range(len(dims))])
    return gain


def scatter_about(own_key, dims, scale, most, cuts=(), kind=jnp.bfloat16):
    gain = steps_of(own_key, dims, cuts, -0.22, 0.18) if cuts else 1.0
    result = jax.random.normal(own_key, dims, jnp.float32) * scale * gain
    return jnp.minimum(jnp.maximum(result, -most), most).astype(kind)


def setup_inputs(seed: int = 0) -> dict:
    seeds = jax.random.split(jax.random.key(seed), 9)
    right_side = scatter_about(seeds[0], (RHS, NPTS), 1.0, 6.0, ((1, 32),), jnp.float32)
    diagonal = jnp.clip(jnp.exp(math.log(4.0) - 2.0794415 * jax.random.uniform(seeds[1], (NPTS,), jnp.float32) ** steps_of(seeds[1], (NPTS,), ((0, 32),), -0.2, 0.2)), 0.5, 4.0)
    tree_order = draw_tree_order(jax.random.fold_in(seeds[8], 71), 0)
    mid_perm = jax.random.permutation(seeds[3], LEAVES).astype(jnp.int32)
    col_factor = scatter_about(seeds[4], (NPTS, LEAVES * RANK), PTS ** -0.5, 0.1875, ((0, 32),))
    mid_factor = scatter_about(seeds[5], (LEAVES * LEAVES * RANK, ROWB * ROWB * RANK), (LEAVES * ROWB * RANK) ** -0.5, 0.15625, ((0, 8), (1, 4)))
    pre_factor = scatter_about(seeds[6], (LEAVES * LEAVES * RANK, ROWB * ROWB * RANK), (LEAVES * ROWB * RANK) ** -0.5, 0.15625, ((0, 8), (1, 4)))
    row_factor = scatter_about(seeds[7], (RANK, NPTS), RANK ** -0.5, 0.875, ((1, 32),))
    return {"right_side": right_side, "diagonal": diagonal, "tree_order": tree_order, "mid_perm": mid_perm, "col_factor": col_factor, "mid_factor": mid_factor, "pre_factor": pre_factor, "row_factor": row_factor}


def gram_apply(field, tree_order, mid_perm, col_factor, mid_weight, row_factor):
    leaves = N_LEAF
    row_count = N_ROWS
    blocks = leaves * row_count
    sides = field.shape[0]
    taken = jnp.take(field, tree_order, axis=1).astype(jnp.bfloat16)
    taken = taken.reshape(sides, blocks, PTS).transpose(1, 0, 2)
    col_blocks = col_factor.reshape(blocks, PTS, leaves * RANK)

    def forward_map(inputs):
        block_field, block_factor = inputs
        return jnp.dot(block_field, block_factor, preferred_element_type=jnp.float32).astype(jnp.bfloat16)

    coeffs = lax.map(forward_map, (taken, col_blocks)).reshape(blocks, sides, leaves, RANK)
    outgoing = coeffs[:, :, mid_perm, :]
    outgoing = outgoing.reshape(leaves, row_count, sides, leaves, RANK).transpose(3, 0, 1, 2, 4)
    mid_blocks = mid_weight.reshape(leaves, leaves, RANK, row_count, row_count * RANK)

    def middle_map(inputs):
        group_coef, group_weight = inputs
        return jnp.einsum('lrsk,lkrm->sm', group_coef.astype(jnp.float32), group_weight.astype(jnp.float32),
                          precision=lax.Precision.HIGHEST)

    head_coef = lax.map(middle_map, (outgoing, mid_blocks))
    head_coef = head_coef.reshape(leaves, sides, row_count, RANK).transpose(0, 2, 1, 3)
    head_coef = head_coef.reshape(blocks, sides, RANK).astype(jnp.bfloat16)
    row_blocks = row_factor.astype(jnp.float32).reshape(RANK, blocks, PTS).transpose(1, 0, 2)
    image_tree = jnp.einsum('bsk,bkn->bsn', head_coef.astype(jnp.float32), row_blocks,
                            precision=lax.Precision.HIGHEST)
    backward = jnp.einsum('bsn,bkn->bsk', image_tree, row_blocks,
                          precision=lax.Precision.HIGHEST).astype(jnp.bfloat16)
    backward = backward.reshape(leaves, row_count, sides, RANK).transpose(0, 2, 1, 3)
    backward = backward.reshape(leaves, sides, row_count * RANK)

    def middle_back(inputs):
        group_back, group_weight = inputs
        return jnp.einsum('sm,lkrm->rlsk', group_back.astype(jnp.float32), group_weight.astype(jnp.float32),
                          precision=lax.Precision.HIGHEST).astype(jnp.bfloat16)

    returned = lax.map(middle_back, (backward, mid_blocks))
    returned = returned.transpose(2, 1, 0, 3, 4).reshape(blocks, leaves, sides, RANK)
    unsent = jnp.zeros_like(returned).at[:, mid_perm].set(returned)

    def backward_map(inputs):
        block_coef, block_factor = inputs
        flattened = block_coef.transpose(1, 0, 2).reshape(sides, leaves * RANK)
        return jnp.dot(flattened, block_factor.T, preferred_element_type=jnp.float32)

    gram_tree = lax.map(backward_map, (unsent, col_blocks))
    gram_tree = gram_tree.transpose(1, 0, 2).reshape(sides, blocks * PTS)
    return jnp.zeros_like(gram_tree).at[:, tree_order].set(gram_tree)


def reference(right_side, diagonal, tree_order, mid_perm, col_factor, mid_factor, pre_factor, row_factor):
    def apply_system(field):
        return diagonal[None, :] * field + gram_apply(field, tree_order, mid_perm, col_factor, mid_factor, row_factor)

    def apply_precond(field):
        return field / diagonal[None, :] + gram_apply(field, tree_order, mid_perm, col_factor, pre_factor, row_factor)

    solution = jnp.zeros_like(right_side)
    residual = right_side
    precond = apply_precond(residual)
    direction = precond
    precond_dot = jnp.sum(residual * precond, axis=1)
    for iteration in range(ITERS):
        image = apply_system(direction)
        alpha_step = precond_dot / jnp.sum(direction * image, axis=1)
        solution = solution + alpha_step[:, None] * direction
        residual = residual - alpha_step[:, None] * image
        if iteration + 1 < ITERS:
            precond = apply_precond(residual)
            dot_next = jnp.sum(residual * precond, axis=1)
            direction = precond + (dot_next / precond_dot)[:, None] * direction
            precond_dot = dot_next
    return solution, residual
```

```python
import functools

import jax
import jax.numpy as jnp
from jax import lax
from jax.experimental import pallas as pl
from jax.experimental.pallas import tpu as pltpu
from jax.sharding import PartitionSpec as P

ITERS = 2
LANES = 128
HALF = 64
BF = jnp.bfloat16
F32 = jnp.float32
MESH = pl.DeviceIdType.MESH


def dot(a, b):
    return jnp.dot(a, b, preferred_element_type=F32)


def dot_t(a, b):
    return lax.dot_general(a, b, (((1,), (1,)), ((), ())), preferred_element_type=F32)


def iota(shape, dim):
    return lax.broadcasted_iota(jnp.int32, shape, dim)


def split3(x):
    hi = x.astype(BF).astype(F32)
    mid = (x - hi).astype(BF).astype(F32)
    return hi, mid, x - hi - mid


def kernel(
    n_leaf, n_rows, rhs_ref, diag_ref, order_ref, perm_ref, col_ref, mid_ref, pre_ref, row_ref,
    sol_ref, res_ref,
    place_ref, colp_ref, cpf_ref, wf_ref, gwt_ref, gall_ref,
    fs_ref, fr_ref, rr_ref, bs_ref, br_ref,
    g_send, g_recv, f_send, f_recv, r_send, r_recv, b_send, b_recv,
):
    leaf = lax.axis_index("leaf")
    row = lax.axis_index("rows")
    sides, points = rhs_ref.shape
    rank = row_ref.shape[0]
    mid_cols = mid_ref.shape[1]
    nm = gall_ref.shape[2]
    pairs = n_leaf // 2
    width = pairs * LANES
    parity = lax.rem(leaf, 2)
    waits = []

    barrier = pltpu.get_barrier_semaphore()
    for d in range(1, n_leaf):
        pl.semaphore_signal(barrier, inc=1, device_id=(lax.rem(leaf + d, n_leaf), row), device_id_type=MESH)
    for d in range(1, n_rows):
        pl.semaphore_signal(barrier, inc=1, device_id=(leaf, lax.rem(row + d, n_rows)), device_id_type=MESH)

    factor = row_ref[...]
    gram = dot_t(factor, factor)
    own_cols = (iota((rank, nm), 1) == row * rank + iota((rank, nm), 0))
    own_cols = jnp.where(own_cols, 1.0, 0.0).astype(BF)
    gram_hi = gram.astype(BF)
    gram_lo = (gram - gram_hi.astype(F32)).astype(BF)
    gall_ref[row] = dot(gram_hi, own_cols) + dot(gram_lo, own_cols)
    pl.semaphore_wait(barrier, n_leaf + n_rows - 2)
    gram_copies = []
    for d in range(1, n_rows):
        copy = pltpu.make_async_remote_copy(
            src_ref=gall_ref.at[row], dst_ref=gall_ref.at[row],
            send_sem=g_send.at[d], recv_sem=g_recv.at[d],
            device_id=(leaf, lax.rem(row + d, n_rows)), device_id_type=MESH,
        )
        copy.start()
        gram_copies.append(copy)
    waits += gram_copies

    cols = iota((1, width), 1)
    group = cols // HALF
    inner = cols % HALF
    target = jnp.where(inner < rank, inner, -n_leaf * rank)
    for q in range(n_leaf):
        target = target + jnp.where(group == q, perm_ref[q] * rank, 0)
    place_rows = 128 if n_leaf * rank % 128 == 0 else rank

    @pl.loop(0, n_leaf * rank // place_rows)
    def _(i):
        start = pl.multiple_of(i * place_rows, place_rows)
        hit = (iota((place_rows, width), 0) + start) == target
        place_ref[pl.ds(start, place_rows), :] = jnp.where(hit, 1.0, 0.0).astype(BF)

    chunk = 256

    @pl.loop(0, points // chunk)
    def _(i):
        start = pl.multiple_of(i * chunk, chunk)
        colp_ref[pl.ds(start, chunk), :] = dot(col_ref[pl.ds(start, chunk), :], place_ref[...]).astype(BF)

    local_order = order_ref[...] - (leaf * n_rows + row) * points

    @pl.loop(0, points // chunk)
    def _(i):
        start = pl.multiple_of(i * chunk, chunk)
        hit = (iota((chunk, points), 0) + start) == local_order
        cpf_ref[pl.ds(start, chunk), :] = dot(jnp.where(hit, 1.0, 0.0).astype(BF), colp_ref[...]).astype(BF)

    lane = iota((sides, LANES), 1)
    inner_lane = lane % HALF

    def lanes_of(value):
        hi, mid, lo = split3(value)
        zero = jnp.zeros((sides, LANES), F32)
        vec = jnp.where(inner_lane == rank, hi, zero)
        vec = jnp.where(inner_lane == rank + 1, mid, vec)
        return jnp.where(inner_lane == rank + 2, lo, vec)

    def build_weights(which, source_ref):
        wf_ref[which] = jnp.zeros(wf_ref.shape[1:], BF)
        extra_shape = (HALF - rank, nm)
        extra = (iota(extra_shape, 0) < 3) & (iota(extra_shape, 1) == mid_cols)
        extra = jnp.where(extra, 1.0, 0.0).astype(BF)
        for l in range(n_leaf):
            start = l * LANES + parity * HALF
            wf_ref[which, pl.ds(pl.multiple_of(start, 16), rank), 0:mid_cols] = source_ref[l * rank:(l + 1) * rank, :]
            wf_ref[which, pl.ds(pl.multiple_of(start + rank, 16), HALF - rank), :] = extra

    def gram_pieces():
        full = gall_ref[...].reshape(n_rows * rank, nm)
        full = jnp.concatenate([full, jnp.zeros((nm - n_rows * rank, nm), F32)], axis=0)
        hi = full.astype(BF)
        return hi, (full - hi.astype(F32)).astype(BF)

    def build_back(which):
        hi, lo = gram_pieces()

        @pl.loop(0, n_leaf * LANES // chunk)
        def _(i):
            start = pl.multiple_of(i * chunk, chunk)
            part = wf_ref[which, pl.ds(start, chunk), :]
            gwt_ref[which, pl.ds(start, chunk), :] = (dot(part, hi) + dot(part, lo)).astype(BF)

    def apply(a, which, field, local_dot, first_window=None, last_window=None):
        coeffs = dot(field.astype(BF), cpf_ref[...])
        tagged = lanes_of(local_dot)
        for j in range(pairs):
            fs_ref[a, j] = (coeffs[:, j * LANES:(j + 1) * LANES] + tagged).astype(BF)
        forward = []
        for d in range(1, n_leaf):
            to = lax.rem(leaf + d, n_leaf)
            copy = pltpu.make_async_remote_copy(
                src_ref=fs_ref.at[a, to // 2], dst_ref=fr_ref.at[a, leaf],
                send_sem=f_send.at[a, d], recv_sem=f_recv.at[a, d],
                device_id=(to, row), device_id_type=MESH,
            )
            copy.start()
            forward.append(copy)
        fr_ref[a, leaf] = fs_ref[a, leaf // 2]
        if first_window is not None:
            first_window()
        for copy in forward:
            copy.wait_recv()
        incoming = jnp.concatenate([fr_ref[a, l] for l in range(n_leaf)], axis=1)
        rr_ref[a, row] = dot(incoming, wf_ref[which])
        across = []
        for d in range(1, n_rows):
            copy = pltpu.make_async_remote_copy(
                src_ref=rr_ref.at[a, row], dst_ref=rr_ref.at[a, row],
                send_sem=r_send.at[a, d], recv_sem=r_recv.at[a, d],
                device_id=(leaf, lax.rem(row + d, n_rows)), device_id_type=MESH,
            )
            copy.start()
            across.append(copy)
        hi, lo = gram_pieces()
        for copy in across:
            copy.wait_recv()
        totals = rr_ref[a, 0]
        for r in range(1, n_rows):
            totals = totals + rr_ref[a, r]
        head = totals.astype(BF)
        back = dot_t(head, gwt_ref[which])
        energy = jnp.sum(head.astype(F32) * (dot(head, hi) + dot(head, lo)), axis=1, keepdims=True)
        tagged = jnp.where(lane // HALF == parity, lanes_of(energy), 0.0)
        for l in range(n_leaf):
            bs_ref[a, l] = (back[:, l * LANES:(l + 1) * LANES] + tagged).astype(BF)
        backward = []
        for d in range(1, n_leaf):
            to = lax.rem(leaf + d, n_leaf)
            copy = pltpu.make_async_remote_copy(
                src_ref=bs_ref.at[a, to], dst_ref=br_ref.at[a, leaf],
                send_sem=b_send.at[a, d], recv_sem=b_recv.at[a, d],
                device_id=(to, row), device_id_type=MESH,
            )
            copy.start()
            backward.append(copy)
        br_ref[a, leaf] = bs_ref[a, leaf]
        if last_window is not None:
            last_window()
        for copy in backward:
            copy.wait_recv()
        tiles = [br_ref[a, 2 * j].astype(F32) + br_ref[a, 2 * j + 1].astype(F32) for j in range(pairs)]
        energies = functools.reduce(jnp.add, tiles)
        energies = jnp.where((inner_lane >= rank) & (inner_lane < rank + 3), energies, 0.0)
        arrived = jnp.concatenate(tiles, axis=1).astype(BF)
        image = dot_t(arrived, cpf_ref[...])
        total_dot = totals[:, mid_cols:mid_cols + 1] + jnp.sum(energies, axis=1, keepdims=True)
        waits.extend(forward + across + backward)
        return image, total_dot

    diagonal = diag_ref[...]
    residual = rhs_ref[...]

    def prepare_first():
        build_weights(0, pre_ref)
        for copy in gram_copies:
            copy.wait_recv()
        build_back(0)

    def prepare_second():
        build_weights(1, mid_ref)
        build_back(1)

    scaled = residual / diagonal
    mapped, rz = apply(0, 0, residual, jnp.sum(residual * scaled, axis=1, keepdims=True), prepare_first, prepare_second)
    direction = scaled + mapped
    solution = jnp.zeros_like(residual)
    for iteration in range(ITERS):
        scaled = diagonal * direction
        mapped, curved = apply(2 * iteration + 1, 1, direction, jnp.sum(direction * scaled, axis=1, keepdims=True))
        alpha = rz / curved
        solution = solution + alpha * direction
        residual = residual - alpha * (scaled + mapped)
        if iteration + 1 < ITERS:
            scaled = residual / diagonal
            mapped, rz_next = apply(2 * iteration + 2, 0, residual, jnp.sum(residual * scaled, axis=1, keepdims=True))
            direction = scaled + mapped + (rz_next / rz) * direction
            rz = rz_next
    sol_ref[...] = solution
    res_ref[...] = residual
    for copy in waits:
        copy.wait_send()


def per_device(n_leaf, n_rows, right_side, diagonal, tree_order, mid_perm, col_factor, mid_factor, pre_factor, row_factor):
    sides, points = right_side.shape
    rank = row_factor.shape[0]
    mid_cols = mid_factor.shape[1]
    nm = (mid_cols // LANES + 1) * LANES
    pairs = n_leaf // 2
    applies = 2 * ITERS
    vmem = pl.BlockSpec(memory_space=pltpu.VMEM)
    dma = pltpu.SemaphoreType.DMA
    return pl.pallas_call(
        functools.partial(kernel, n_leaf, n_rows),
        out_shape=(
            jax.ShapeDtypeStruct((sides, points), F32),
            jax.ShapeDtypeStruct((sides, points), F32),
        ),
        in_specs=[vmem, vmem, vmem, pl.BlockSpec(memory_space=pltpu.SMEM), vmem, vmem, vmem, vmem],
        out_specs=(vmem, vmem),
        scratch_shapes=[
            pltpu.VMEM((n_leaf * rank, pairs * LANES), BF),
            pltpu.VMEM((points, pairs * LANES), BF),
            pltpu.VMEM((points, pairs * LANES), BF),
            pltpu.VMEM((2, n_leaf * LANES, nm), BF),
            pltpu.VMEM((2, n_leaf * LANES, nm), BF),
            pltpu.VMEM((n_rows, rank, nm), F32),
            pltpu.VMEM((applies, pairs, sides, LANES), BF),
            pltpu.VMEM((applies, n_leaf, sides, LANES), BF),
            pltpu.VMEM((applies, n_rows, sides, nm), F32),
            pltpu.VMEM((applies, n_leaf, sides, LANES), BF),
            pltpu.VMEM((applies, n_leaf, sides, LANES), BF),
            dma((n_rows,)), dma((n_rows,)),
            dma((applies, n_leaf)), dma((applies, n_leaf)),
            dma((applies, n_rows)), dma((applies, n_rows)),
            dma((applies, n_leaf)), dma((applies, n_leaf)),
        ],
        compiler_params=pltpu.CompilerParams(collective_id=0, has_side_effects=True),
    )(
        right_side, diagonal.reshape(1, points), tree_order.reshape(1, points), mid_perm,
        col_factor, mid_factor, pre_factor, row_factor,
    )


def solution(mesh):
    both = ("leaf", "rows")
    return jax.shard_map(
        functools.partial(per_device, mesh.shape["leaf"], mesh.shape["rows"]),
        mesh=mesh,
        in_specs=(
            P(None, both), P(both), P(both), P(), P(both, None),
            P("leaf", "rows"), P("leaf", "rows"), P(None, both),
        ),
        out_specs=(P(None, both), P(None, both)),
        check_vma=False,
    )
```

```python
import functools

import jax
import jax.numpy as jnp
from jax import lax
from jax.experimental import pallas as pl
from jax.experimental.pallas import tpu as pltpu
from jax.sharding import PartitionSpec as P

ITERS = 2
LANES = 128
HALF = 64
BF = jnp.bfloat16
F32 = jnp.float32
MESH = pl.DeviceIdType.MESH
CHUNK = 512


def dot(a, b):
    return jnp.dot(a, b, preferred_element_type=F32)


def dot_t(a, b):
    return lax.dot_general(a, b, (((1,), (1,)), ((), ())), preferred_element_type=F32)


def iota(shape, dim):
    return lax.broadcasted_iota(jnp.int32, shape, dim)


def split3(x):
    hi = x.astype(BF).astype(F32)
    mid = (x - hi).astype(BF).astype(F32)
    return hi, mid, x - hi - mid


def kernel(
    n_leaf, n_rows, rhs_ref, diag_ref, order_ref, perm_ref, col_ref, mid_ref, pre_ref, row_ref,
    sol_ref, res_ref,
    place_ref, colp_ref, cpf_ref, cpb_ref, spread_ref, wf_ref, wb_ref, gall_ref, gram_ref,
    fs_ref, fr_ref, rr_ref, bs_ref, br_ref,
    g_send, g_recv, f_send, f_recv, r_send, r_recv, b_send, b_recv,
):
    leaf = lax.axis_index("leaf")
    row = lax.axis_index("rows")
    sides, points = rhs_ref.shape
    rank = row_ref.shape[0]
    mid_cols = mid_ref.shape[0]
    nm = gall_ref.shape[2]
    pairs = n_leaf // 2
    width = pairs * LANES
    parity = lax.rem(leaf, 2)
    waits = []

    barrier = pltpu.get_barrier_semaphore()
    for d in range(1, n_leaf):
        pl.semaphore_signal(barrier, inc=1, device_id=(lax.rem(leaf + d, n_leaf), row), device_id_type=MESH)
    for d in range(1, n_rows):
        pl.semaphore_signal(barrier, inc=1, device_id=(leaf, lax.rem(row + d, n_rows)), device_id_type=MESH)

    factor = row_ref[...]
    gram = dot_t(factor, factor)
    own_cols = (iota((rank, nm), 1) == row * rank + iota((rank, nm), 0))
    own_cols = jnp.where(own_cols, 1.0, 0.0).astype(BF)
    gram_hi = gram.astype(BF)
    gram_lo = (gram - gram_hi.astype(F32)).astype(BF)
    gall_ref[row] = dot(gram_hi, own_cols) + dot(gram_lo, own_cols)
    cols = iota((1, width), 1)
    group = cols // HALF
    inner = cols % HALF
    target = jnp.where(inner < rank, inner, -n_leaf * rank)
    for q in range(n_leaf):
        target = target + jnp.where(group == q, perm_ref[q] * rank, 0)
    place_rows = 128 if n_leaf * rank % 128 == 0 else rank

    @pl.loop(0, n_leaf * rank // place_rows)
    def _(i):
        start = pl.multiple_of(i * place_rows, place_rows)
        hit = (iota((place_rows, width), 0) + start) == target
        place_ref[pl.ds(start, place_rows), :] = jnp.where(hit, 1.0, 0.0).astype(BF)

    chunk = min(CHUNK, points)

    @pl.loop(0, points // chunk)
    def _(i):
        start = pl.multiple_of(i * chunk, chunk)
        colp_ref[pl.ds(start, chunk), :] = dot(col_ref[pl.ds(start, chunk), :], place_ref[...]).astype(BF)

    local_order = order_ref[...] - (leaf * n_rows + row) * points

    @pl.loop(0, points // chunk)
    def _(i):
        start = pl.multiple_of(i * chunk, chunk)
        hit = (iota((chunk, points), 0) + start) == local_order
        cpf_ref[pl.ds(start, chunk), :] = dot(jnp.where(hit, 1.0, 0.0).astype(BF), colp_ref[...]).astype(BF)

    pl.semaphore_wait(barrier, n_leaf + n_rows - 2)
    gram_copies = []
    for d in range(1, n_rows):
        copy = pltpu.make_async_remote_copy(
            src_ref=gall_ref.at[row], dst_ref=gall_ref.at[row],
            send_sem=g_send.at[d], recv_sem=g_recv.at[d],
            device_id=(leaf, lax.rem(row + d, n_rows)), device_id_type=MESH,
        )
        copy.start()
        gram_copies.append(copy)
    waits += gram_copies

    lane = iota((sides, LANES), 1)
    inner_lane = lane % HALF

    def lanes_of(value):
        hi, mid, lo = split3(value)
        zero = jnp.zeros((sides, LANES), F32)
        vec = jnp.where(inner_lane == rank, hi, zero)
        vec = jnp.where(inner_lane == rank + 1, mid, vec)
        return jnp.where(inner_lane == rank + 2, lo, vec)

    def build_spread():
        cols = iota((1, n_leaf * LANES), 1)
        inner = cols % HALF
        target = jnp.where((inner < rank) & ((cols % LANES) // HALF == parity), (cols // LANES) * rank + inner, -1)

        @pl.loop(0, n_leaf * rank // place_rows)
        def _(i):
            start = pl.multiple_of(i * place_rows, place_rows)
            hit = (iota((place_rows, n_leaf * LANES), 0) + start) == target
            spread_ref[pl.ds(start, place_rows), :] = jnp.where(hit, 1.0, 0.0).astype(BF)

    def build_weights(which, source_ref):
        spread = dot(source_ref[...], spread_ref[...]).astype(BF)
        shape = (nm - mid_cols, n_leaf * LANES)
        cols = iota(shape, 1)
        inner = cols % HALF
        extra = (iota(shape, 0) == 0) & ((cols % LANES) // HALF == parity) & (inner >= rank) & (inner < rank + 3)
        extra = jnp.where(extra, 1.0, 0.0).astype(BF)
        full = jnp.concatenate([spread, extra], axis=0)
        wf_ref[which] = full

    def build_gram():
        full = gall_ref[...].reshape(n_rows * rank, nm)
        full = jnp.concatenate([full, jnp.zeros((nm - n_rows * rank, nm), F32)], axis=0)
        hi = full.astype(BF)
        gram_ref[0] = hi
        gram_ref[1] = (full - hi.astype(F32)).astype(BF)

    def build_back(which):
        part = wf_ref[which]
        wb_ref[which] = (dot(gram_ref[0], part) + dot(gram_ref[1], part)).astype(BF)

    def apply(a, which, field, local_dot, windows=None):
        coeffs = dot(field.astype(BF), cpf_ref[...])
        tagged = lanes_of(local_dot)
        for j in range(pairs):
            fs_ref[a, j] = (coeffs[:, j * LANES:(j + 1) * LANES] + tagged).astype(BF)
        forward = []
        for d in range(1, n_leaf):
            to = lax.rem(leaf + d, n_leaf)
            copy = pltpu.make_async_remote_copy(
                src_ref=fs_ref.at[a, to // 2], dst_ref=fr_ref.at[a, leaf],
                send_sem=f_send.at[a, d], recv_sem=f_recv.at[a, d],
                device_id=(to, row), device_id_type=MESH,
            )
            copy.start()
            forward.append(copy)
        fr_ref[a, leaf] = fs_ref[a, leaf // 2]
        if windows is not None:
            windows[0]()
        for copy in forward:
            copy.wait_recv()
        incoming = jnp.concatenate([fr_ref[a, l] for l in range(n_leaf)], axis=1)
        rr_ref[a, row] = dot_t(incoming, wf_ref[which])
        across = []
        for d in range(1, n_rows):
            copy = pltpu.make_async_remote_copy(
                src_ref=rr_ref.at[a, row], dst_ref=rr_ref.at[a, row],
                send_sem=r_send.at[a, d], recv_sem=r_recv.at[a, d],
                device_id=(leaf, lax.rem(row + d, n_rows)), device_id_type=MESH,
            )
            copy.start()
            across.append(copy)
        if windows is not None:
            windows[1]()
        for copy in across:
            copy.wait_recv()
        totals = rr_ref[a, 0]
        for r in range(1, n_rows):
            totals = totals + rr_ref[a, r]
        head = totals.astype(BF)
        back = dot(head, wb_ref[which])
        energy = jnp.sum(head.astype(F32) * dot(head, gram_ref[0]), axis=1, keepdims=True)
        tagged = jnp.where(lane // HALF == parity, lanes_of(energy), 0.0)
        for l in range(n_leaf):
            bs_ref[a, l] = (back[:, l * LANES:(l + 1) * LANES] + tagged).astype(BF)
        backward = []
        for d in range(1, n_leaf):
            to = lax.rem(leaf + d, n_leaf)
            copy = pltpu.make_async_remote_copy(
                src_ref=bs_ref.at[a, to], dst_ref=br_ref.at[a, leaf],
                send_sem=b_send.at[a, d], recv_sem=b_recv.at[a, d],
                device_id=(to, row), device_id_type=MESH,
            )
            copy.start()
            backward.append(copy)
        br_ref[a, leaf] = bs_ref[a, leaf]
        if windows is not None:
            windows[2]()
        for copy in backward:
            copy.wait_recv()
        tiles = [br_ref[a, 2 * j].astype(F32) + br_ref[a, 2 * j + 1].astype(F32) for j in range(pairs)]
        energies = functools.reduce(jnp.add, tiles)
        energies = jnp.where((inner_lane >= rank) & (inner_lane < rank + 3), energies, 0.0)
        arrived = jnp.concatenate(tiles, axis=1).astype(BF)
        image = dot(arrived, cpb_ref[...])
        total_dot = totals[:, mid_cols:mid_cols + 1] + jnp.sum(energies, axis=1, keepdims=True)
        waits.extend(forward + across + backward)
        return image, total_dot

    diagonal = diag_ref[...]
    residual = rhs_ref[...]

    def first_window():
        build_spread()
        build_weights(0, pre_ref)

    def second_window():
        for copy in gram_copies:
            copy.wait_recv()
        build_gram()
        build_back(0)

    def third_window():
        cpb_ref[...] = cpf_ref[...].T
        build_weights(1, mid_ref)
        build_back(1)

    windows = (first_window, second_window, third_window)
    scaled = residual / diagonal
    mapped, rz = apply(0, 0, residual, jnp.sum(residual * scaled, axis=1, keepdims=True), windows)
    direction = scaled + mapped
    solution = jnp.zeros_like(residual)
    for iteration in range(ITERS):
        scaled = diagonal * direction
        mapped, curved = apply(2 * iteration + 1, 1, direction, jnp.sum(direction * scaled, axis=1, keepdims=True))
        alpha = rz / curved
        solution = solution + alpha * direction
        residual = residual - alpha * (scaled + mapped)
        if iteration + 1 < ITERS:
            scaled = residual / diagonal
            mapped, rz_next = apply(2 * iteration + 2, 0, residual, jnp.sum(residual * scaled, axis=1, keepdims=True))
            direction = scaled + mapped + (rz_next / rz) * direction
            rz = rz_next
    sol_ref[...] = solution
    res_ref[...] = residual
    for copy in waits:
        copy.wait_send()


def per_device(n_leaf, n_rows, right_side, diagonal, tree_order, mid_perm, col_factor, mid_factor, pre_factor, row_factor):
    sides, points = right_side.shape
    rank = row_factor.shape[0]
    mid_factor, pre_factor = mid_factor.T, pre_factor.T
    mid_cols = mid_factor.shape[0]
    nm = (mid_cols // LANES + 1) * LANES
    pairs = n_leaf // 2
    applies = 2 * ITERS
    vmem = pl.BlockSpec(memory_space=pltpu.VMEM)
    dma = pltpu.SemaphoreType.DMA
    return pl.pallas_call(
        functools.partial(kernel, n_leaf, n_rows),
        out_shape=(
            jax.ShapeDtypeStruct((sides, points), F32),
            jax.ShapeDtypeStruct((sides, points), F32),
        ),
        in_specs=[vmem, vmem, vmem, pl.BlockSpec(memory_space=pltpu.SMEM), vmem, vmem, vmem, vmem],
        out_specs=(vmem, vmem),
        scratch_shapes=[
            pltpu.VMEM((n_leaf * rank, pairs * LANES), BF),
            pltpu.VMEM((points, pairs * LANES), BF),
            pltpu.VMEM((points, pairs * LANES), BF),
            pltpu.VMEM((pairs * LANES, points), BF),
            pltpu.VMEM((n_leaf * rank, n_leaf * LANES), BF),
            pltpu.VMEM((2, nm, n_leaf * LANES), BF),
            pltpu.VMEM((2, nm, n_leaf * LANES), BF),
            pltpu.VMEM((n_rows, rank, nm), F32),
            pltpu.VMEM((2, nm, nm), BF),
            pltpu.VMEM((applies, pairs, sides, LANES), BF),
            pltpu.VMEM((applies, n_leaf, sides, LANES), BF),
            pltpu.VMEM((applies, n_rows, sides, nm), F32),
            pltpu.VMEM((applies, n_leaf, sides, LANES), BF),
            pltpu.VMEM((applies, n_leaf, sides, LANES), BF),
            dma((n_rows,)), dma((n_rows,)),
            dma((applies, n_leaf)), dma((applies, n_leaf)),
            dma((applies, n_rows)), dma((applies, n_rows)),
            dma((applies, n_leaf)), dma((applies, n_leaf)),
        ],
        compiler_params=pltpu.CompilerParams(collective_id=0, has_side_effects=True),
    )(
        right_side, diagonal.reshape(1, points), tree_order.reshape(1, points), mid_perm,
        col_factor, mid_factor, pre_factor, row_factor,
    )


def solution(mesh):
    both = ("leaf", "rows")
    return jax.shard_map(
        functools.partial(per_device, mesh.shape["leaf"], mesh.shape["rows"]),
        mesh=mesh,
        in_specs=(
            P(None, both), P(both), P(both), P(), P(both, None),
            P("leaf", "rows"), P("leaf", "rows"), P(None, both),
        ),
        out_specs=(P(None, both), P(None, both)),
        check_vma=False,
    )
```

```python
import functools

import jax
import jax.numpy as jnp
from jax import lax
from jax.experimental import pallas as pl
from jax.experimental.pallas import tpu as pltpu
from jax.sharding import PartitionSpec as P

ITERS = 2
LANES = 128
HALF = 64
BF = jnp.bfloat16
F32 = jnp.float32
MESH = pl.DeviceIdType.MESH
CHUNK = 512


def dot(a, b):
    return jnp.dot(a, b, preferred_element_type=F32)


def dot_t(a, b):
    return lax.dot_general(a, b, (((1,), (1,)), ((), ())), preferred_element_type=F32)


def iota(shape, dim):
    return lax.broadcasted_iota(jnp.int32, shape, dim)


def split3(x):
    hi = x.astype(BF).astype(F32)
    mid = (x - hi).astype(BF).astype(F32)
    return hi, mid, x - hi - mid


def kernel(
    n_leaf, n_rows, rhs_ref, diag_ref, order_ref, perm_ref, col_hbm, mid_ref, pre_ref, row_ref,
    sol_ref, res_ref,
    col_ref, col_sem, place_ref, colp_ref, cpf_ref, cpb_ref, spread_ref, wf_ref, wb_ref, gall_ref, gram_ref,
    fs_ref, fr_ref, rr_ref, bs_ref, br_ref,
    g_send, g_recv, f_send, f_recv, r_send, r_recv, b_send, b_recv,
):
    leaf = lax.axis_index("leaf")
    row = lax.axis_index("rows")
    sides, points = rhs_ref.shape
    rank = row_ref.shape[0]
    mid_cols = mid_ref.shape[0]
    nm = gall_ref.shape[2]
    pairs = n_leaf // 2
    width = pairs * LANES
    parity = lax.rem(leaf, 2)
    waits = []

    col_copy = pltpu.make_async_copy(col_hbm, col_ref, col_sem)
    col_copy.start()
    barrier = pltpu.get_barrier_semaphore()
    for d in range(1, n_leaf):
        pl.semaphore_signal(barrier, inc=1, device_id=(lax.rem(leaf + d, n_leaf), row), device_id_type=MESH)
    for d in range(1, n_rows):
        pl.semaphore_signal(barrier, inc=1, device_id=(leaf, lax.rem(row + d, n_rows)), device_id_type=MESH)

    factor = row_ref[...]
    gram = dot_t(factor, factor)
    own_cols = (iota((rank, nm), 1) == row * rank + iota((rank, nm), 0))
    own_cols = jnp.where(own_cols, 1.0, 0.0).astype(BF)
    gram_hi = gram.astype(BF)
    gram_lo = (gram - gram_hi.astype(F32)).astype(BF)
    gall_ref[row] = dot(gram_hi, own_cols) + dot(gram_lo, own_cols)
    cols = iota((1, width), 1)
    group = cols // HALF
    inner = cols % HALF
    target = jnp.where(inner < rank, inner, -n_leaf * rank)
    for q in range(n_leaf):
        target = target + jnp.where(group == q, perm_ref[q] * rank, 0)
    place_rows = 128 if n_leaf * rank % 128 == 0 else rank

    @pl.loop(0, n_leaf * rank // place_rows)
    def _(i):
        start = pl.multiple_of(i * place_rows, place_rows)
        hit = (iota((place_rows, width), 0) + start) == target
        place_ref[pl.ds(start, place_rows), :] = jnp.where(hit, 1.0, 0.0).astype(BF)

    chunk = min(CHUNK, points)
    col_copy.wait()

    @pl.loop(0, points // chunk)
    def _(i):
        start = pl.multiple_of(i * chunk, chunk)
        colp_ref[pl.ds(start, chunk), :] = dot(col_ref[pl.ds(start, chunk), :], place_ref[...]).astype(BF)

    local_order = order_ref[...] - (leaf * n_rows + row) * points

    @pl.loop(0, points // chunk)
    def _(i):
        start = pl.multiple_of(i * chunk, chunk)
        hit = (iota((chunk, points), 0) + start) == local_order
        cpf_ref[pl.ds(start, chunk), :] = dot(jnp.where(hit, 1.0, 0.0).astype(BF), colp_ref[...]).astype(BF)

    pl.semaphore_wait(barrier, n_leaf + n_rows - 2)
    gram_copies = []
    for d in range(1, n_rows):
        copy = pltpu.make_async_remote_copy(
            src_ref=gall_ref.at[row], dst_ref=gall_ref.at[row],
            send_sem=g_send.at[d], recv_sem=g_recv.at[d],
            device_id=(leaf, lax.rem(row + d, n_rows)), device_id_type=MESH,
        )
        copy.start()
        gram_copies.append(copy)
    waits += gram_copies

    lane = iota((sides, LANES), 1)
    inner_lane = lane % HALF

    def lanes_of(value):
        hi, mid, lo = split3(value)
        zero = jnp.zeros((sides, LANES), F32)
        vec = jnp.where(inner_lane == rank, hi, zero)
        vec = jnp.where(inner_lane == rank + 1, mid, vec)
        return jnp.where(inner_lane == rank + 2, lo, vec)

    def build_spread():
        cols = iota((1, n_leaf * LANES), 1)
        inner = cols % HALF
        target = jnp.where((inner < rank) & ((cols % LANES) // HALF == parity), (cols // LANES) * rank + inner, -1)

        @pl.loop(0, n_leaf * rank // place_rows)
        def _(i):
            start = pl.multiple_of(i * place_rows, place_rows)
            hit = (iota((place_rows, n_leaf * LANES), 0) + start) == target
            spread_ref[pl.ds(start, place_rows), :] = jnp.where(hit, 1.0, 0.0).astype(BF)

    def build_weights(which, source_ref):
        spread = dot(source_ref[...], spread_ref[...]).astype(BF)
        shape = (nm - mid_cols, n_leaf * LANES)
        cols = iota(shape, 1)
        inner = cols % HALF
        extra = (iota(shape, 0) == 0) & ((cols % LANES) // HALF == parity) & (inner >= rank) & (inner < rank + 3)
        extra = jnp.where(extra, 1.0, 0.0).astype(BF)
        full = jnp.concatenate([spread, extra], axis=0)
        wf_ref[which] = full

    def build_gram():
        full = gall_ref[...].reshape(n_rows * rank, nm)
        full = jnp.concatenate([full, jnp.zeros((nm - n_rows * rank, nm), F32)], axis=0)
        hi = full.astype(BF)
        gram_ref[0] = hi
        gram_ref[1] = (full - hi.astype(F32)).astype(BF)

    def build_back(which):
        part = wf_ref[which]
        wb_ref[which] = (dot(gram_ref[0], part) + dot(gram_ref[1], part)).astype(BF)

    def apply(a, which, field, local_dot, windows=None):
        coeffs = dot(field.astype(BF), cpf_ref[...])
        tagged = lanes_of(local_dot)
        for j in range(pairs):
            fs_ref[a, j] = (coeffs[:, j * LANES:(j + 1) * LANES] + tagged).astype(BF)
        forward = []
        for d in range(1, n_leaf):
            to = lax.rem(leaf + d, n_leaf)
            copy = pltpu.make_async_remote_copy(
                src_ref=fs_ref.at[a, to // 2], dst_ref=fr_ref.at[a, leaf],
                send_sem=f_send.at[a, d], recv_sem=f_recv.at[a, d],
                device_id=(to, row), device_id_type=MESH,
            )
            copy.start()
            forward.append(copy)
        fr_ref[a, leaf] = fs_ref[a, leaf // 2]
        if windows is not None:
            windows[0]()
        for copy in forward:
            copy.wait_recv()
        incoming = jnp.concatenate([fr_ref[a, l] for l in range(n_leaf)], axis=1)
        rr_ref[a, row] = dot_t(incoming, wf_ref[which])
        across = []
        for d in range(1, n_rows):
            copy = pltpu.make_async_remote_copy(
                src_ref=rr_ref.at[a, row], dst_ref=rr_ref.at[a, row],
                send_sem=r_send.at[a, d], recv_sem=r_recv.at[a, d],
                device_id=(leaf, lax.rem(row + d, n_rows)), device_id_type=MESH,
            )
            copy.start()
            across.append(copy)
        if windows is not None:
            windows[1]()
        for copy in across:
            copy.wait_recv()
        totals = rr_ref[a, 0]
        for r in range(1, n_rows):
            totals = totals + rr_ref[a, r]
        head = totals.astype(BF)
        back = dot(head, wb_ref[which])
        energy = jnp.sum(head.astype(F32) * dot(head, gram_ref[0]), axis=1, keepdims=True)
        tagged = jnp.where(lane // HALF == parity, lanes_of(energy), 0.0)
        for l in range(n_leaf):
            bs_ref[a, l] = (back[:, l * LANES:(l + 1) * LANES] + tagged).astype(BF)
        backward = []
        for d in range(1, n_leaf):
            to = lax.rem(leaf + d, n_leaf)
            copy = pltpu.make_async_remote_copy(
                src_ref=bs_ref.at[a, to], dst_ref=br_ref.at[a, leaf],
                send_sem=b_send.at[a, d], recv_sem=b_recv.at[a, d],
                device_id=(to, row), device_id_type=MESH,
            )
            copy.start()
            backward.append(copy)
        br_ref[a, leaf] = bs_ref[a, leaf]
        if windows is not None:
            windows[2]()
        for copy in backward:
            copy.wait_recv()
        tiles = [br_ref[a, 2 * j].astype(F32) + br_ref[a, 2 * j + 1].astype(F32) for j in range(pairs)]
        energies = functools.reduce(jnp.add, tiles)
        energies = jnp.where((inner_lane >= rank) & (inner_lane < rank + 3), energies, 0.0)
        arrived = jnp.concatenate(tiles, axis=1).astype(BF)
        image = dot(arrived, cpb_ref[...])
        total_dot = totals[:, mid_cols:mid_cols + 1] + jnp.sum(energies, axis=1, keepdims=True)
        waits.extend(forward + across + backward)
        return image, total_dot

    diagonal = diag_ref[...]
    residual = rhs_ref[...]

    def first_window():
        build_spread()
        build_weights(0, pre_ref)

    def second_window():
        for copy in gram_copies:
            copy.wait_recv()
        build_gram()
        build_back(0)

    def third_window():
        cpb_ref[...] = cpf_ref[...].T

    windows = (first_window, second_window, third_window)
    later_windows = (lambda: build_weights(1, mid_ref), lambda: build_back(1), lambda: None)
    scaled = residual / diagonal
    mapped, rz = apply(0, 0, residual, jnp.sum(residual * scaled, axis=1, keepdims=True), windows)
    direction = scaled + mapped
    solution = jnp.zeros_like(residual)
    for iteration in range(ITERS):
        scaled = diagonal * direction
        local_dot = jnp.sum(direction * scaled, axis=1, keepdims=True)
        mapped, curved = apply(2 * iteration + 1, 1, direction, local_dot, later_windows if iteration == 0 else None)
        alpha = rz / curved
        solution = solution + alpha * direction
        residual = residual - alpha * (scaled + mapped)
        if iteration + 1 < ITERS:
            scaled = residual / diagonal
            mapped, rz_next = apply(2 * iteration + 2, 0, residual, jnp.sum(residual * scaled, axis=1, keepdims=True))
            direction = scaled + mapped + (rz_next / rz) * direction
            rz = rz_next
    sol_ref[...] = solution
    res_ref[...] = residual
    for copy in waits:
        copy.wait_send()


def per_device(n_leaf, n_rows, right_side, diagonal, tree_order, mid_perm, col_factor, mid_factor, pre_factor, row_factor):
    sides, points = right_side.shape
    rank = row_factor.shape[0]
    mid_factor, pre_factor = mid_factor.T, pre_factor.T
    mid_cols = mid_factor.shape[0]
    nm = (mid_cols // LANES + 1) * LANES
    pairs = n_leaf // 2
    applies = 2 * ITERS
    vmem = pl.BlockSpec(memory_space=pltpu.VMEM)
    dma = pltpu.SemaphoreType.DMA
    return pl.pallas_call(
        functools.partial(kernel, n_leaf, n_rows),
        out_shape=(
            jax.ShapeDtypeStruct((sides, points), F32),
            jax.ShapeDtypeStruct((sides, points), F32),
        ),
        in_specs=[vmem, vmem, vmem, pl.BlockSpec(memory_space=pltpu.SMEM), pl.BlockSpec(memory_space=pl.ANY), vmem, vmem, vmem],
        out_specs=(vmem, vmem),
        scratch_shapes=[
            pltpu.VMEM(col_factor.shape, BF),
            dma,
            pltpu.VMEM((n_leaf * rank, pairs * LANES), BF),
            pltpu.VMEM((points, pairs * LANES), BF),
            pltpu.VMEM((points, pairs * LANES), BF),
            pltpu.VMEM((pairs * LANES, points), BF),
            pltpu.VMEM((n_leaf * rank, n_leaf * LANES), BF),
            pltpu.VMEM((2, nm, n_leaf * LANES), BF),
            pltpu.VMEM((2, nm, n_leaf * LANES), BF),
            pltpu.VMEM((n_rows, rank, nm), F32),
            pltpu.VMEM((2, nm, nm), BF),
            pltpu.VMEM((applies, pairs, sides, LANES), BF),
            pltpu.VMEM((applies, n_leaf, sides, LANES), BF),
            pltpu.VMEM((applies, n_rows, sides, nm), F32),
            pltpu.VMEM((applies, n_leaf, sides, LANES), BF),
            pltpu.VMEM((applies, n_leaf, sides, LANES), BF),
            dma((n_rows,)), dma((n_rows,)),
            dma((applies, n_leaf)), dma((applies, n_leaf)),
            dma((applies, n_rows)), dma((applies, n_rows)),
            dma((applies, n_leaf)), dma((applies, n_leaf)),
        ],
        compiler_params=pltpu.CompilerParams(collective_id=0, has_side_effects=True),
    )(
        right_side, diagonal.reshape(1, points), tree_order.reshape(1, points), mid_perm,
        col_factor, mid_factor, pre_factor, row_factor,
    )


def solution(mesh):
    both = ("leaf", "rows")
    return jax.shard_map(
        functools.partial(per_device, mesh.shape["leaf"], mesh.shape["rows"]),
        mesh=mesh,
        in_specs=(
            P(None, both), P(both), P(both), P(), P(both, None),
            P("leaf", "rows"), P("leaf", "rows"), P(None, both),
        ),
        out_specs=(P(None, both), P(None, both)),
        check_vma=False,
    )
```
